32 devices in a mesh: mat: 4 (over x, core), frac: 8 (over z, y).
Axes of the slice: x: 2, y: 2, z: 4, core: 2. Of those that a mesh axis runs over, the one named last changes fastest.
Arguments:
- pressure_start: float32 [64, 512, 256], P('mat', 'frac'), may hold values from -6 to 6
- face_trans: float32 [3, 64, 512, 256], P(None, 'mat', 'frac'), may hold values from 0.2 to 2
- cell_coef: float32 [64, 512, 256], P('mat', 'frac'), may hold values from 0.05 to 0.5
- matrix_source: float32 [64, 512, 256], P('mat', 'frac'), may hold values from -6 to 6
- mortar_owner: int32 [16384, 1], P(('mat', 'frac')), may hold values from 0 to 31; in each aligned block of 512 rows (0 to 511, 512 to 1023, ...) at most 32 rows name the same one
- mortar_cell: int32 [16384], P(('mat', 'frac')), may hold values from 0 to 262143
- mortar_frac: int32 [16384], P(('mat', 'frac')), may hold values from 0 to 8191
- mortar_kappa: float32 [16384], P(('mat', 'frac')), may hold values from 0.5 to 2
- tiles: float32 [64, 4, 128, 128], P('frac'), may hold values from -0.25 to 0.25
- tile_cols: int32 [64, 4], P('frac'), may hold values from 0 to 63
- frac_diag: float32 [8192], P('frac'), may hold values from 4 to 8
- frac_source: float32 [8192], P('frac'), may hold values from -6 to 6
- fracture_start: float32 [8192], P('frac'), may hold values from -6 to 6
Outputs:
- pressure: float32 [64, 512, 256], P('mat', 'frac')
- fracture: float32 [8192], P('frac')
- flux: float32 [16384], P(('mat', 'frac'))
The draws below stay inside these ranges and needn't reach their ends.
Inputs may be any that keep to these rules, and one draw needn't show every extreme that they name: `mortar_owner`: among the 512 mortar cells of one device, at most 32 name the same owner, and in some devices some owner is named exactly 32 times.
All inputs are finite; a program needn't handle non-finite values.
Results may differ from the reference program's by a relative error of at most 0.00015.
Values sent between devices are 32-bit elements; how exact they have to be, the bound alone decides.
A program may use at most 128 MiB of HBM per device.

```python
import math
import jax
import jax.numpy as jnp
import numpy as np
from jax import lax

CX = 16
CY = 64
CZ = 256
MORT_DEV = 512
B = 128
TILES = 4
SWEEPS = 2
CG_ITERS = 3
OUTER = 2
NX = 64
NY = 512
CELLS = 262144
NB = 64
NF = 8192
M = 16384
CAP = 32
N_MAT = 4
N_FRAC = 8
DEVICES = 32


def set_ends(values, key, low, high):
    longest = values.shape.index(max(values.shape))
    spots = []
    for shift in (0, 1):
        where = [jax.random.randint(jax.random.fold_in(key, axis), (), 0, length) for axis, length in enumerate(values.shape)]
        where[longest] = (where[longest] + shift) % values.shape[longest]
        spots.append(tuple(where))
    return values.at[spots[0]].set(low).at[spots[1]].set(high)


def block_levels(own_key, shape, pieces, smallest, top_value):
    level = 1.0
    for dim, parts in pieces:
        draws = jax.random.uniform(jax.random.fold_in(jax.random.fold_in(own_key, 6), dim), (parts,), jnp.float32, smallest / len(pieces), top_value / len(pieces))
        level = level * jnp.repeat(jnp.exp(draws), shape[dim] // parts).reshape((-1,) + (1,) * (len(shape) - 1 - dim))
    return level


def shared_out(rng, own, number, rows, amount, top, most, slope):
    order = jax.random.permutation(rng, amount)
    crowded, ordinary = shares(amount, rows * top, most, slope, True), shares(amount, rows * top, most, slope, False)
    places = jnp.arange(amount)

    def named(lengths, turn):
        used = int((lengths > 0).sum())
        fixed = max(1, used // 4)
        moved = fixed + (places - fixed + turn * (used - fixed)) % max(1, amount - fixed)
        return jnp.zeros((amount,), jnp.int32).at[order[jnp.where(places < fixed, places, moved)]].set(jnp.asarray(lengths, jnp.int32))

    lengths = jnp.where(number % 4 == 0, named(crowded, number // 4), named(ordinary, number - number // 4 - 1))
    mixed = jax.random.permutation(jax.random.fold_in(own, 3), amount)
    donor, taker = mixed[0:amount // 2 * 2:2], mixed[1:amount // 2 * 2:2]
    slack = jnp.minimum(lengths[donor] - 1, most - lengths[taker]) // 2
    slack = jnp.where((donor == order[0]) | (taker == order[0]) | (lengths[taker] == 0), 0, jnp.maximum(slack, 0))
    moved = jax.random.randint(jax.random.fold_in(own, 4), (amount // 2,), 0, 1 << 20) % (slack + 1)
    lengths = lengths.at[donor].add(-moved).at[taker].add(moved)
    labels = jnp.searchsorted(jnp.cumsum(lengths), jnp.arange(rows * top), side="right").astype(jnp.int32)
    grid = labels.reshape(top, rows).T
    grid = grid[jax.random.permutation(jax.random.fold_in(own, 1), rows)]
    turn = jax.random.randint(jax.random.fold_in(own, 2), (rows, 1), 0, top)
    return jnp.take_along_axis(grid, (jnp.arange(top)[None, :] + turn) % top, axis=1)


def shares(count, total, limit, lean, full):
    portions = [(1 << 20) // math.isqrt(standing ** lean) + 1 for standing in range(1, count + 1)]
    largest = limit if full else min(limit, max(-(-total // count), total * portions[0] // sum(portions)))
    least = 1 if total - largest >= count - 1 else 0
    given, surplus = [largest] + [least] * (count - 1), total - largest - least * (count - 1)
    while surplus > 0:
        movable = [i for i in range(1, count) if given[i] < largest] or [i for i in range(1, count) if given[i] < limit]
        whole, left = sum([portions[i] for i in movable]), surplus
        for i in movable:
            addition = min(limit - given[i], max(1, left * portions[i] // whole), surplus)
            given[i] = given[i] + addition
            surplus = surplus - addition
    return np.array(given)


def normal_values(rng, extent, scale, limit, split=(), dtype=jnp.bfloat16):
    values = scale * jax.random.normal(rng, extent, jnp.float32)
    if split:
        values = values * block_levels(rng, extent, split, -0.22, 0.18)
    return jnp.clip(values, -limit, limit).astype(dtype)


def setup_inputs(seed: int = 0) -> dict:
    seeds = jax.random.split(jax.random.key(seed), 14)
    pressure_start = normal_values(seeds[0], (NX, NY, CZ), 1.0, 6.0, ((0, 4), (1, 8)), jnp.float32)
    face_trans = jnp.clip(jnp.exp(math.log(2.0) - 2.3025851 * jax.random.uniform(seeds[1], (3, NX, NY, CZ), jnp.float32) ** block_levels(seeds[1], (3, NX, NY, CZ), ((1, 4), (2, 8)), -0.2, 0.2)), 0.2, 2.0)
    cell_coef = jnp.clip(jnp.exp(math.log(0.5) - 2.3025851 * jax.random.uniform(seeds[2], (NX, NY, CZ), jnp.float32) ** block_levels(seeds[2], (NX, NY, CZ), ((0, 4), (1, 8)), -0.2, 0.2)), 0.05, 0.5)
    matrix_source = normal_values(seeds[3], (NX, NY, CZ), 1.0, 6.0, ((0, 4), (1, 8)), jnp.float32)
    mortar_owner_keys = jax.random.split(jax.random.fold_in(seeds[4], 1), M // MORT_DEV)
    mortar_owner_turns = jax.random.permutation(jax.random.fold_in(seeds[4], 3), M // MORT_DEV)
    mortar_owner = jax.vmap(lambda own, number: shared_out(jax.random.fold_in(seeds[4], 2), own, number, MORT_DEV, DEVICES, 1, CAP, 2))(mortar_owner_keys, mortar_owner_turns).reshape((M, 1))
    mortar_cell = set_ends(jax.random.randint(seeds[5], (M,), 0, CELLS), jax.random.fold_in(seeds[5], 1), 0, CELLS - 1).astype(jnp.int32)
    mortar_frac = set_ends(jax.random.randint(seeds[6], (M,), 0, NF), jax.random.fold_in(seeds[6], 1), 0, NF - 1).astype(jnp.int32)
    mortar_kappa = jnp.clip(jnp.exp(math.log(2.0) - 1.3862944 * jax.random.uniform(seeds[7], (M,), jnp.float32) ** block_levels(seeds[7], (M,), ((0, 32),), -0.2, 0.2)), 0.5, 2.0)
    tiles = normal_values(seeds[8], (NB, TILES, B, B), (TILES * B) ** -0.5, 0.25, ((0, 8),), jnp.float32)
    tile_cols = set_ends(jax.random.randint(seeds[9], (NB, TILES), 0, NB), jax.random.fold_in(seeds[9], 1), 0, NB - 1).astype(jnp.int32)
    frac_diag = jnp.clip(jnp.exp(math.log(8.0) - 0.6931472 * jax.random.uniform(seeds[10], (NF,), jnp.float32) ** block_levels(seeds[10], (NF,), ((0, 8),), -0.2, 0.2)), 4.0, 8.0)
    frac_source = normal_values(seeds[11], (NF,), 1.0, 6.0, ((0, 8),), jnp.float32)
    fracture_start = normal_values(seeds[12], (NF,), 1.0, 6.0, ((0, 8),), jnp.float32)
    return {"pressure_start": pressure_start, "face_trans": face_trans, "cell_coef": cell_coef, "matrix_source": matrix_source, "mortar_owner": mortar_owner, "mortar_cell": mortar_cell, "mortar_frac": mortar_frac, "mortar_kappa": mortar_kappa, "tiles": tiles, "tile_cols": tile_cols, "frac_diag": frac_diag, "frac_source": frac_source, "fracture_start": fracture_start}


relax_weight = 0.8


def shift_next(values, along):
    padding = [(0, 0)] * values.ndim
    padding[along] = (0, 1)
    return lax.slice_in_dim(jnp.pad(values, padding), 1, values.shape[along] + 1, axis=along)


def shift_prev(values, along):
    padding = [(0, 0)] * values.ndim
    padding[along] = (1, 0)
    return lax.slice_in_dim(jnp.pad(values, padding), 0, values.shape[along], axis=along)


def relax_grid(pressure, face_trans, cell_coef, matrix_source, source):
    tx_low = shift_prev(face_trans[0], 0)
    ty_low = shift_prev(face_trans[1], 1)
    tz_low = shift_prev(face_trans[2], 2)
    diagonal = cell_coef + face_trans[0] + tx_low + face_trans[1] + ty_low + face_trans[2] + tz_low
    applied = (diagonal * pressure - face_trans[0] * shift_next(pressure, 0) - tx_low * shift_prev(pressure, 0)
               - face_trans[1] * shift_next(pressure, 1) - ty_low * shift_prev(pressure, 1)
               - face_trans[2] * shift_next(pressure, 2) - tz_low * shift_prev(pressure, 2))
    return pressure + relax_weight * (matrix_source + source - applied) / diagonal


def fracture_apply(vector, tiles, tile_cols, frac_diag):
    size_b = tiles.shape[2]
    blocks = vector.reshape(-1, size_b)
    forward = jnp.einsum("rtij,rtj->ri", tiles, blocks[tile_cols], precision=lax.Precision.HIGHEST)
    backward = jnp.einsum("rtij,ri->rtj", tiles, blocks, precision=lax.Precision.HIGHEST)
    spread = jnp.zeros_like(blocks).at[tile_cols.reshape(-1)].add(backward.reshape(-1, size_b))
    return frac_diag * vector + 0.5 * (forward + spread).reshape(-1)


def reference(pressure_start, face_trans, cell_coef, matrix_source, mortar_owner, mortar_cell, mortar_frac, mortar_kappa, tiles, tile_cols, frac_diag, frac_source, fracture_start):
    cells = CX * CY * CZ
    pressure = pressure_start
    fracture = fracture_start
    place = mortar_owner[:, 0].astype(jnp.int32) * cells + mortar_cell.astype(jnp.int32)
    flux = jnp.zeros(mortar_kappa.shape, jnp.float32)
    for outer_no in range(OUTER):
        by_device = pressure.reshape(N_MAT, CX, N_FRAC, CY, CZ).transpose(0, 2, 1, 3, 4).reshape(-1)
        trace = by_device[place]
        flux = mortar_kappa * (trace - fracture[mortar_frac])
        load = jnp.zeros(fracture.shape, jnp.float32).at[mortar_frac].add(flux)
        target = frac_source + load
        residual = target - fracture_apply(fracture, tiles, tile_cols, frac_diag)
        direction = residual
        norm_now = jnp.sum(residual * residual)
        for step in range(CG_ITERS):
            image = fracture_apply(direction, tiles, tile_cols, frac_diag)
            alpha = norm_now / jnp.sum(direction * image)
            fracture = fracture + alpha * direction
            residual = residual - alpha * image
            norm_next = jnp.sum(residual * residual)
            direction = residual + (norm_next / norm_now) * direction
            norm_now = norm_next
        landed = jnp.zeros(by_device.shape, jnp.float32).at[place].add(flux)
        source = landed.reshape(N_MAT, N_FRAC, CX, CY, CZ).transpose(0, 2, 1, 3, 4).reshape(pressure.shape)
        for sweep_no in range(SWEEPS):
            pressure = relax_grid(pressure, face_trans, cell_coef, matrix_source, source)
    return pressure, fracture, flux
```

```python
import functools

import jax
import jax.numpy as jnp
from jax import lax
from jax.experimental import pallas as pl
from jax.experimental.pallas import tpu as pltpu
from jax.sharding import PartitionSpec as P

SWEEPS = 2
CG_ITERS = 3
OUTER = 2

EXACT = lax.Precision.HIGHEST
MESH = pl.DeviceIdType.MESH

relax_weight = 0.8


def shifted(value, axis, steps):
    count = lax.axis_size(axis)
    leading, last = (max(0, -steps), min(count, count - steps))
    return lax.ppermute(value, axis, [(source, source + steps) for source in range(leading, last)])


def with_halo(block, sides, width):
    for axis, dim in sides:
        count = lax.axis_size(axis)
        forward = [(i, i + 1) for i in range(count - 1)]
        backward = [(target, source) for source, target in forward]
        low = lax.ppermute(
            lax.slice_in_dim(block, block.shape[dim] - width, None, axis=dim), axis, forward
        )
        high = lax.ppermute(lax.slice_in_dim(block, 0, width, axis=dim), axis, backward)
        block = jnp.concatenate([low, block, high], axis=dim)
    return block


def shift_next(values, along):
    padding = [(0, 0)] * values.ndim
    padding[along] = (0, 1)
    return lax.slice_in_dim(jnp.pad(values, padding), 1, values.shape[along] + 1, axis=along)


def shift_prev(values, along):
    padding = [(0, 0)] * values.ndim
    padding[along] = (1, 0)
    return lax.slice_in_dim(jnp.pad(values, padding), 0, values.shape[along], axis=along)


def relax(padded, coef_part, source_part, inside):
    centre = padded[1:-1, 1:-1]
    tx_here = coef_part[0, 1:-1, 1:-1]
    tx_low = coef_part[0, :-2, 1:-1]
    ty_here = coef_part[1, 1:-1, 1:-1]
    ty_low = coef_part[1, 1:-1, :-2]
    tz_here = coef_part[2, 1:-1, 1:-1]
    tz_low = shift_prev(tz_here, 2)
    cell_part = coef_part[3, 1:-1, 1:-1]
    base_part = coef_part[4, 1:-1, 1:-1]
    diagonal = cell_part + tx_here + tx_low + ty_here + ty_low + tz_here + tz_low
    diagonal = jnp.where(inside, diagonal, 1.0)
    applied = (
        diagonal * centre
        - tx_here * padded[2:, 1:-1]
        - tx_low * padded[:-2, 1:-1]
        - ty_here * padded[1:-1, 2:]
        - ty_low * padded[1:-1, :-2]
        - tz_here * shift_next(centre, 2)
        - tz_low * shift_prev(centre, 2)
    )
    updated = centre + relax_weight * (base_part + source_part - applied) / diagonal
    return jnp.where(inside, updated, 0.0)


def fracture_kernel(first, n_frac, n_mat, *refs):
    if first:
        (trace_ref, kappa_ref, place_ref, tiles_ref, cols_ref, cols_row_ref, diag_ref, begin_ref, source_ref,
         flux_ref, full_ref, resid_ref, load_ref, *scratch) = refs
    else:
        (trace_ref, kappa_ref, place_ref, tiles_ref, cols_ref, cols_row_ref, diag_ref, begin_ref, before_ref, loaded_ref,
         flux_ref, own_ref, *scratch) = refs
    gather_ref, outgo_ref, income_ref, mat_ref, back_ref, forth_ref, sems = *scratch[:6], scratch[6:]
    gather_send, gather_recv, part_send, part_recv, mat_send, mat_recv = sems
    rows, tiles_row = tiles_ref.shape[0], tiles_ref.shape[1]
    size_b = tiles_ref.shape[3]
    blocks = rows * n_frac
    me = lax.axis_index("frac")
    me_mat = lax.axis_index("mat")
    mine = pl.ds(pl.multiple_of(me * rows, rows), rows)

    barrier = pltpu.get_barrier_semaphore()
    for k in range(1, n_frac):
        pl.semaphore_signal(barrier, inc=1, device_id={"frac": lax.rem(me + k, n_frac)}, device_id_type=MESH)
    for k in range(1, n_mat):
        pl.semaphore_signal(barrier, inc=1, device_id={"mat": lax.rem(me_mat + k, n_mat)}, device_id_type=MESH)
    pl.semaphore_wait(barrier, n_frac + n_mat - 2)

    sent = []

    def gather(phase, value):
        gather_ref[phase, mine, :] = value
        copies = []
        for k in range(1, n_frac):
            copy = pltpu.make_async_remote_copy(
                src_ref=gather_ref.at[phase, mine],
                dst_ref=gather_ref.at[phase, mine],
                send_sem=gather_send.at[phase, k - 1],
                recv_sem=gather_recv.at[phase, k - 1],
                device_id={"frac": lax.rem(me + k, n_frac)},
                device_id_type=MESH,
            )
            copy.start()
            copies.append(copy)
        sent.extend(copies)
        return copies

    def exchange(phase, low, high):
        part = pl.ds(low, high - low)
        copies = []
        for k in range(1, n_frac):
            target = lax.rem(me + k, n_frac)
            copy = pltpu.make_async_remote_copy(
                src_ref=outgo_ref.at[phase, target, part],
                dst_ref=income_ref.at[phase, me, part],
                send_sem=part_send.at[phase, k - 1],
                recv_sem=part_recv.at[phase, k - 1],
                device_id={"frac": target},
                device_id_type=MESH,
            )
            copy.start()
            copies.append(copy)
        sent.extend(copies)
        income_ref[phase, me, part, :] = outgo_ref[phase, me, part, :]
        for copy in copies:
            copy.wait_recv()
        total = income_ref[phase, 0, part, :]
        for k in range(1, n_frac):
            total = total + income_ref[phase, k, part, :]
        return total

    def products(phase, with_back):
        def row(r, carry):
            across = gather_ref[phase, pl.ds(me * rows + r, 1), :]
            down = jnp.broadcast_to(across, (size_b, size_b)).T
            total = jnp.zeros((size_b, size_b), jnp.float32)
            for t in range(tiles_row):
                tile = tiles_ref[r, t]
                total = total + tile * gather_ref[phase, pl.ds(cols_ref[r, t], 1), :]
                if with_back:
                    back_ref[pl.ds(r * tiles_row + t, 1), :] = jnp.sum(tile * down, axis=0, keepdims=True)
            forth_ref[pl.ds(r, 1), :] = jnp.sum(total.T, axis=0, keepdims=True)
            return carry

        lax.fori_loop(0, rows, row, 0)
        forward = forth_ref[...]
        if not with_back:
            return forward, None
        named = lax.broadcasted_iota(jnp.int32, (blocks, rows * tiles_row), 0) == cols_row_ref[...]
        spread = jnp.dot(named.astype(jnp.float32), back_ref[...], precision=EXACT, preferred_element_type=jnp.float32)
        return forward, spread

    def total_of(values):
        return jnp.sum(values, axis=(0, 1), keepdims=True)

    diag = diag_ref[...]
    place = place_ref[...]
    slots = place.shape[1]
    block_of = place // size_b
    lane_of = place - block_of * size_b
    by_block = (lax.broadcasted_iota(jnp.int32, (blocks, slots), 0) == block_of).astype(jnp.float32)
    by_lane = (lax.broadcasted_iota(jnp.int32, (size_b, slots), 0) == lane_of).astype(jnp.float32)

    def fluxes(full):
        picked = lax.dot_general(full, by_block, (((0,), (0,)), ((), ())), precision=EXACT, preferred_element_type=jnp.float32)
        at_slots = jnp.sum(picked * by_lane, axis=0, keepdims=True)
        flux = kappa_ref[...] * (trace_ref[...] - at_slots)
        flux_ref[...] = flux
        return lax.dot_general(by_block * flux, by_lane, (((1,), (1,)), ((), ())), precision=EXACT, preferred_element_type=jnp.float32)

    if first:
        begin = begin_ref[...]
        for copy in gather(0, begin):
            copy.wait_recv()
        fracture = gather_ref[0]
        landed = fluxes(fracture)
        forward, spread = products(0, True)
        for k in range(n_frac):
            outgo_ref[0, k, 0:rows, :] = spread[k * rows : (k + 1) * rows]
            outgo_ref[0, k, rows : 2 * rows, :] = landed[k * rows : (k + 1) * rows]
        both = exchange(0, 0, 2 * rows)
        image = diag * begin + 0.5 * (forward + both[0:rows])
        part_load = both[rows : 2 * rows]
    else:
        fracture = begin_ref[...]
        landed = fluxes(fracture)
        for k in range(n_frac):
            outgo_ref[0, k, rows : 2 * rows, :] = landed[k * rows : (k + 1) * rows]
        part_load = exchange(0, rows, 2 * rows)
    mat_ref[me_mat] = part_load
    copies = []
    for k in range(1, n_mat):
        copy = pltpu.make_async_remote_copy(
            src_ref=mat_ref.at[me_mat],
            dst_ref=mat_ref.at[me_mat],
            send_sem=mat_send.at[k - 1],
            recv_sem=mat_recv.at[k - 1],
            device_id={"mat": lax.rem(me_mat + k, n_mat)},
            device_id_type=MESH,
        )
        copy.start()
        copies.append(copy)
    sent.extend(copies)
    for copy in copies:
        copy.wait_recv()
    load = mat_ref[0]
    for k in range(1, n_mat):
        load = load + mat_ref[k]
    if first:
        load_ref[...] = load
        residual = source_ref[...] + load - image
    else:
        residual = before_ref[...] + (load - loaded_ref[...])

    for step in range(CG_ITERS):
        phase = step + 1
        needed = first or step + 1 < CG_ITERS
        for copy in gather(phase, residual):
            copy.wait_recv()
        whole = gather_ref[phase]
        forward, spread = products(phase, needed)
        inner = residual * (diag * residual + forward)
        for k in range(n_frac):
            if needed:
                outgo_ref[phase, k, 0:rows, :] = spread[k * rows : (k + 1) * rows]
            outgo_ref[phase, k, rows : 2 * rows, :] = inner
        both = exchange(phase, 0 if needed else rows, 2 * rows)
        if needed:
            image = diag * residual + 0.5 * (forward + both[0:rows])
            product = total_of(both[rows : 2 * rows])
        else:
            product = total_of(both)
        norm_next = total_of(whole * whole)
        if step == 0:
            alpha = norm_next / product
            direction = whole
            along = image
        else:
            ratio = norm_next / norm_now
            alpha = norm_next / (product - ratio * norm_next / alpha)
            direction = whole + ratio * direction
            if needed:
                along = image + ratio * along
        norm_now = norm_next
        fracture = fracture + alpha * direction
        if needed:
            residual = residual - alpha * along
    if first:
        full_ref[...] = fracture
        resid_ref[...] = residual
    else:
        gather_ref[0] = fracture
        own_ref[...] = gather_ref[0, mine, :]
    for copy in sent:
        copy.wait_send()


def fracture_step(first, trace, kappa, place, tiles, tile_cols, diag, *extra):
    n_frac, n_mat = lax.axis_size("frac"), lax.axis_size("mat")
    rows, tiles_row, size_b = tiles.shape[0], tiles.shape[1], tiles.shape[3]
    blocks = rows * n_frac
    own = jax.ShapeDtypeStruct((rows, size_b), jnp.float32)
    full = jax.ShapeDtypeStruct((blocks, size_b), jnp.float32)
    vmem = pl.BlockSpec(memory_space=pltpu.VMEM)
    smem = pl.BlockSpec(memory_space=pltpu.SMEM)
    phases = CG_ITERS + 1
    outs = (trace_shape(trace), full, own, own) if first else (trace_shape(trace), own)
    return pl.pallas_call(
        functools.partial(fracture_kernel, first, n_frac, n_mat),
        out_shape=outs,
        in_specs=[vmem] * 4 + [smem] + [vmem] * (2 + len(extra)),
        out_specs=(vmem,) * len(outs),
        scratch_shapes=[
            pltpu.VMEM((phases, blocks, size_b), jnp.float32),
            pltpu.VMEM((phases, n_frac, 2 * rows, size_b), jnp.float32),
            pltpu.VMEM((phases, n_frac, 2 * rows, size_b), jnp.float32),
            pltpu.VMEM((n_mat, rows, size_b), jnp.float32),
            pltpu.VMEM((rows * tiles_row, size_b), jnp.float32),
            pltpu.VMEM((rows, size_b), jnp.float32),
            pltpu.SemaphoreType.DMA((phases, n_frac - 1)),
            pltpu.SemaphoreType.DMA((phases, n_frac - 1)),
            pltpu.SemaphoreType.DMA((phases, n_frac - 1)),
            pltpu.SemaphoreType.DMA((phases, n_frac - 1)),
            pltpu.SemaphoreType.DMA((n_mat - 1,)),
            pltpu.SemaphoreType.DMA((n_mat - 1,)),
        ],
        compiler_params=pltpu.CompilerParams(collective_id=0 if first else 1, has_side_effects=True),
        name="fracture_first" if first else "fracture_next",
    )(trace, kappa, place, tiles, tile_cols, tile_cols.reshape(1, -1), diag, *extra)


def trace_shape(trace):
    return jax.ShapeDtypeStruct(trace.shape, jnp.float32)


def body(
    pressure_start,
    face_trans,
    cell_coef,
    matrix_source,
    mortar_owner,
    mortar_cell,
    mortar_frac,
    mortar_kappa,
    tiles,
    tile_cols,
    frac_diag,
    frac_source,
    fracture_start,
):
    width_x, width_y, depth_z = pressure_start.shape
    cells = width_x * width_y * depth_z
    mat_count = lax.axis_size("mat")
    frac_count = lax.axis_size("frac")
    devices = mat_count * frac_count
    row_mat = lax.axis_index("mat")
    row_frac = lax.axis_index("frac")
    size_b = tiles.shape[2]
    coefs = jnp.concatenate([face_trans, cell_coef[None], matrix_source[None]], 0)
    lower_x = shifted(face_trans[0, -1], "mat", 1)
    lower_y = shifted(face_trans[1, :, -1], "frac", 1)
    coef_ext = jnp.pad(coefs, ((0, 0), (1, 1), (1, 1), (0, 0)))
    coef_ext = coef_ext.at[0, 0, 1:-1].set(lower_x)
    coef_ext = coef_ext.at[1, 1:-1, 0].set(lower_y)
    owner = mortar_owner[:, 0]
    mortar_count = owner.shape[0]
    capacity = max(2, 2 * mortar_count // devices)
    hits = (owner[:, None] == jnp.arange(devices, dtype=jnp.int32)[None, :]).astype(jnp.int32)
    ranks = jnp.cumsum(hits, axis=0)
    slot = jnp.sum(ranks * hits, axis=1) - 1
    place = owner * capacity + slot
    slots = devices * capacity
    at_slot = (place[:, None] == jnp.arange(slots, dtype=jnp.int32)[None, :]).astype(jnp.float32)
    payload = jnp.stack([mortar_cell.astype(jnp.float32), mortar_frac.astype(jnp.float32), mortar_kappa])
    outgoing = jnp.dot(payload, at_slot, precision=EXACT).reshape(3, devices, capacity)
    incoming = lax.all_to_all(outgoing, ("mat", "frac"), split_axis=1, concat_axis=1, tiled=True)
    cell_slots = jnp.round(incoming[0]).astype(jnp.int32).reshape(-1)
    frac_slots = jnp.round(incoming[1]).astype(jnp.int32).reshape(1, -1)
    kappa_slots = incoming[2].reshape(1, -1)
    diag = frac_diag.reshape(-1, size_b)
    pressure = pressure_start
    fracture = fracture_start.reshape(-1, size_b)
    global_x = row_mat * width_x - 0 + jnp.arange(width_x)
    global_y = row_frac * width_y - 0 + jnp.arange(width_y)
    inside = (
        ((global_x >= 0) & (global_x < width_x * mat_count))[:, None]
        & ((global_y >= 0) & (global_y < width_y * frac_count))[None, :]
    )[:, :, None]
    for outer_no in range(OUTER):
        trace = pressure.reshape(-1)[cell_slots].reshape(1, -1)
        common = (trace, kappa_slots, frac_slots, tiles, tile_cols, diag)
        if outer_no == 0:
            flux, full, residual, load = fracture_step(True, *common, fracture, frac_source.reshape(-1, size_b))
        else:
            flux, fracture = fracture_step(False, *common, full, residual, load)
        source = jax.ops.segment_sum(flux.reshape(-1), cell_slots, num_segments=cells).reshape(pressure.shape)
        for sweep_no in range(SWEEPS):
            padded = with_halo(pressure, (("mat", 0), ("frac", 1)), 1)
            pressure = relax(padded, coef_ext, source, inside)
    returned = lax.all_to_all(
        flux.reshape(devices, capacity), ("mat", "frac"), split_axis=0, concat_axis=0, tiled=True
    )
    return (pressure, fracture.reshape(-1), returned.reshape(-1)[place])


def solution(mesh):
    in_specs = (
        P("mat", "frac", None),
        P(None, "mat", "frac", None),
        P("mat", "frac", None),
        P("mat", "frac", None),
        P(("mat", "frac"), None),
        P(("mat", "frac")),
        P(("mat", "frac")),
        P(("mat", "frac")),
        P("frac", None, None, None),
        P("frac", None),
        P("frac"),
        P("frac"),
        P("frac"),
    )
    out_specs = (P("mat", "frac", None), P("frac"), P(("mat", "frac")))
    return jax.shard_map(body, mesh=mesh, in_specs=in_specs, out_specs=out_specs, check_vma=False)
```

```python
import functools

import jax
import jax.numpy as jnp
from jax import lax
from jax.experimental import pallas as pl
from jax.experimental.pallas import tpu as pltpu
from jax.sharding import PartitionSpec as P

SWEEPS = 2
CG_ITERS = 3
OUTER = 2

EXACT = lax.Precision.HIGHEST
MESH = pl.DeviceIdType.MESH

relax_weight = 0.8


def coupled_kernel(n_frac, n_mat, *refs):
    (press_ref, face_ref, cell_ref, msource_ref, where_ref, kappa_ref, place_ref, tiles_ref, cols_ref, cols_row_ref,
     diag_ref, begin_ref, fsource_ref, out_ref, own_ref, flux_ref, *scratch) = refs
    (gather_ref, outgo_ref, income_ref, mat_ref, back_ref, forth_ref, grid_ref, tx_ref, inv_ref, base_ref, row_hot_ref,
     lane_hot_ref, side_ref, edge_ref, ty_edge_ref, ty_side_ref, gather_send, gather_recv, part_send, part_recv,
     mat_send, mat_recv, halo_send, halo_recv) = scratch
    rows, tiles_row = tiles_ref.shape[0], tiles_ref.shape[1]
    size_b = tiles_ref.shape[3]
    width_x, width_y, depth_z = press_ref.shape
    slots = place_ref.shape[1]
    blocks = rows * n_frac
    sweeps = OUTER * SWEEPS
    phases = CG_ITERS + 1
    me = lax.axis_index("frac")
    me_mat = lax.axis_index("mat")
    mine = pl.ds(pl.multiple_of(me * rows, rows), rows)

    barrier = pltpu.get_barrier_semaphore()
    for k in range(1, n_frac):
        pl.semaphore_signal(barrier, inc=1, device_id={"frac": lax.rem(me + k, n_frac)}, device_id_type=MESH)
    for k in range(1, n_mat):
        pl.semaphore_signal(barrier, inc=1, device_id={"mat": lax.rem(me_mat + k, n_mat)}, device_id_type=MESH)
    pl.semaphore_wait(barrier, n_frac + n_mat - 2)

    sent = []
    pieces = []

    def fill(count):
        for _ in range(min(count, len(pieces))):
            pieces.pop(0)()

    def send(src, dst, send_sem, recv_sem, device):
        copy = pltpu.make_async_remote_copy(
            src_ref=src, dst_ref=dst, send_sem=send_sem, recv_sem=recv_sem, device_id=device, device_id_type=MESH
        )
        copy.start()
        sent.append(copy)
        return copy

    def gather(phase, value):
        gather_ref[phase, mine, :] = value
        here = gather_ref.at[phase, mine]
        return [
            send(here, here, gather_send.at[phase, k - 1], gather_recv.at[phase, k - 1], {"frac": lax.rem(me + k, n_frac)})
            for k in range(1, n_frac)
        ]

    def exchange(phase, low, high, count):
        part = pl.ds(low, high - low)
        copies = []
        for k in range(1, n_frac):
            target = lax.rem(me + k, n_frac)
            copies.append(
                send(
                    outgo_ref.at[phase, target, part],
                    income_ref.at[phase, me, part],
                    part_send.at[phase, k - 1],
                    part_recv.at[phase, k - 1],
                    {"frac": target},
                )
            )
        income_ref[phase, me, part, :] = outgo_ref[phase, me, part, :]
        fill(count)
        for copy in copies:
            copy.wait_recv()
        total = income_ref[phase, 0, part, :]
        for k in range(1, n_frac):
            total = total + income_ref[phase, k, part, :]
        return total

    def products(phase, with_back):
        def row(r, carry):
            across = gather_ref[phase, pl.ds(me * rows + r, 1), :]
            down = jnp.broadcast_to(across, (size_b, size_b)).T
            total = jnp.zeros((size_b, size_b), jnp.float32)
            for t in range(tiles_row):
                tile = tiles_ref[r, t]
                total = total + tile * gather_ref[phase, pl.ds(cols_ref[r, t], 1), :]
                if with_back:
                    back_ref[pl.ds(r * tiles_row + t, 1), :] = jnp.sum(tile * down, axis=0, keepdims=True)
            forth_ref[pl.ds(r, 1), :] = jnp.sum(total.T, axis=0, keepdims=True)
            return carry

        lax.fori_loop(0, rows, row, 0)
        forward = forth_ref[...]
        if not with_back:
            return forward, None
        named = lax.broadcasted_iota(jnp.int32, (blocks, rows * tiles_row), 0) == cols_row_ref[...]
        spread = jnp.dot(named.astype(jnp.float32), back_ref[...], precision=EXACT, preferred_element_type=jnp.float32)
        return forward, spread

    def total_of(values):
        return jnp.sum(values, axis=(0, 1), keepdims=True)

    def thirds(values):
        high = values.astype(jnp.bfloat16)
        rest = values - high.astype(jnp.float32)
        middle = rest.astype(jnp.bfloat16)
        return high, middle, (rest - middle.astype(jnp.float32)).astype(jnp.bfloat16)

    lanes = lax.broadcasted_iota(jnp.int32, (width_y, depth_z), 1)
    lines = lax.broadcasted_iota(jnp.int32, (width_y, depth_z), 0)
    next_mat, prev_mat = lax.rem(me_mat + 1, n_mat), lax.rem(me_mat + n_mat - 1, n_mat)
    next_frac, prev_frac = lax.rem(me + 1, n_frac), lax.rem(me + n_frac - 1, n_frac)
    halos = {}

    def send_halo(sweep, last, first):
        sems = [(halo_send.at[sweep, d], halo_recv.at[sweep, d]) for d in range(4)]
        halos[sweep] = [
            send(last, grid_ref.at[sweep, 0], *sems[0], {"mat": next_mat}),
            send(first, grid_ref.at[sweep, width_x + 1], *sems[1], {"mat": prev_mat}),
            send(edge_ref.at[sweep, 0], side_ref.at[sweep, 0], *sems[2], {"frac": next_frac}),
            send(edge_ref.at[sweep, 1], side_ref.at[sweep, 1], *sems[3], {"frac": prev_frac}),
        ]

    def wait_halo(sweep):
        for copy in halos[sweep]:
            copy.wait_recv()
        grid_ref[sweep, 0] = jnp.where(me_mat == 0, 0.0, grid_ref[sweep, 0])
        grid_ref[sweep, width_x + 1] = jnp.where(me_mat == n_mat - 1, 0.0, grid_ref[sweep, width_x + 1])
        side_ref[sweep, 0] = jnp.where(me == 0, 0.0, side_ref[sweep, 0])
        side_ref[sweep, 1] = jnp.where(me == n_frac - 1, 0.0, side_ref[sweep, 1])

    def tz_inner(x):
        return jnp.where(lanes == depth_z - 1, 0.0, face_ref[2, x])

    def set_inverse():
        for copy in coef_copies:
            copy.wait_recv()
        tx_ref[0] = jnp.where(me_mat == 0, 0.0, tx_ref[0])
        ty_side_ref[...] = jnp.where(me == 0, 0.0, ty_side_ref[...])

        def plane(x, carry):
            tx_here, ty_here = face_ref[0, x], face_ref[1, x]
            tx_ref[x + 1] = tx_here
            ty_low = jnp.where(lines == 0, ty_side_ref[pl.ds(x, 1), :], pltpu.roll(ty_here, 1, 0))
            tz_low = pltpu.roll(tz_inner(x), 1, 1)
            inv_ref[x] = relax_weight / (cell_ref[x] + tx_here + tx_ref[x] + ty_here + ty_low + face_ref[2, x] + tz_low)
            return carry

        lax.fori_loop(0, width_x, plane, 0)

    def sweep_part(sweep, low, high):
        def plane(x, carry):
            here = grid_ref[sweep, x + 1]
            ty_here, tz_here = face_ref[1, x], tz_inner(x)
            up = jnp.where(lines == width_y - 1, side_ref[sweep, 1, pl.ds(x, 1), :], pltpu.roll(here, width_y - 1, 0))
            down = jnp.where(
                lines == 0,
                ty_side_ref[pl.ds(x, 1), :] * side_ref[sweep, 0, pl.ds(x, 1), :],
                pltpu.roll(ty_here * here, 1, 0),
            )
            total = base_ref[x] + tx_ref[x + 1] * grid_ref[sweep, x + 2] + tx_ref[x] * grid_ref[sweep, x]
            total = total + ty_here * up + down
            total = total + tz_here * pltpu.roll(here, depth_z - 1, 1) + pltpu.roll(tz_here * here, 1, 1)
            value = (1.0 - relax_weight) * here + inv_ref[x] * total
            if sweep + 1 < sweeps:
                grid_ref[sweep + 1, x + 1] = value
                edge_ref[sweep + 1, 0, pl.ds(x, 1), :] = value[width_y - 1 :]
                edge_ref[sweep + 1, 1, pl.ds(x, 1), :] = value[:1]
            else:
                out_ref[x] = value
            return carry

        lax.fori_loop(low, high, plane, 0)

    quarter = width_x // 4

    def set_sources(low, parts):
        hot = row_hot_ref[low * width_y : (low + quarter) * width_y, :]
        total = sum(
            lax.dot_general(hot, part, (((1,), (1,)), ((), ())), preferred_element_type=jnp.float32) for part in parts
        )
        base_ref[low : low + quarter] = msource_ref[low : low + quarter] + total.reshape(quarter, width_y, depth_z)

    def add_sweep(sweep):
        pieces.append(lambda: wait_halo(sweep))
        for q in range(4):
            pieces.append(functools.partial(sweep_part, sweep, q * quarter, (q + 1) * quarter))
        if sweep + 1 < sweeps:
            pieces.append(
                lambda: send_halo(sweep + 1, grid_ref.at[sweep + 1, width_x], grid_ref.at[sweep + 1, 1])
            )

    def traces(sweep):
        found = []
        cut = slots // 4
        parts = thirds(grid_ref[sweep, 1 : width_x + 1].reshape(width_x * width_y, depth_z))
        for q in range(4):
            hot = row_hot_ref[:, q * cut : (q + 1) * cut]
            picked = sum(
                lax.dot_general(part, hot, (((0,), (0,)), ((), ())), preferred_element_type=jnp.float32)
                for part in parts
            )
            mask = lane_hot_ref[:, q * cut : (q + 1) * cut].astype(jnp.float32)
            found.append(jnp.sum(picked * mask, axis=0, keepdims=True))
        return jnp.concatenate(found, axis=1)

    begin = begin_ref[...]
    first_copies = gather(0, begin)
    grid_ref[0, 1 : width_x + 1] = press_ref[...]
    edge_ref[0, 0] = press_ref[:, width_y - 1, :]
    edge_ref[0, 1] = press_ref[:, 0, :]
    ty_edge_ref[...] = face_ref[1, :, width_y - 1, :]
    coef_copies = [
        send(face_ref.at[0, width_x - 1], tx_ref.at[0], halo_send.at[sweeps, 0], halo_recv.at[sweeps, 0], {"mat": next_mat}),
        send(ty_edge_ref, ty_side_ref, halo_send.at[sweeps, 2], halo_recv.at[sweeps, 2], {"frac": next_frac}),
    ]
    send_halo(0, press_ref.at[width_x - 1], press_ref.at[0])
    place = place_ref[...]
    block_of = place // size_b
    lane_of = place - block_of * size_b
    by_block = (lax.broadcasted_iota(jnp.int32, (blocks, slots), 0) == block_of).astype(jnp.float32)
    by_lane = (lax.broadcasted_iota(jnp.int32, (size_b, slots), 0) == lane_of).astype(jnp.float32)
    cell = where_ref[...]
    cell_row = cell // depth_z
    cell_lane = cell - cell_row * depth_z

    row_hot_ref[...] = (lax.broadcasted_iota(jnp.int32, row_hot_ref.shape, 0) == cell_row).astype(jnp.float32).astype(jnp.bfloat16)
    lane_hot_ref[...] = (lax.broadcasted_iota(jnp.int32, lane_hot_ref.shape, 0) == cell_lane).astype(jnp.float32).astype(jnp.bfloat16)

    diag = diag_ref[...]
    for outer_no in range(OUTER):
        first = outer_no == 0
        stage = outer_no * phases
        trace = traces(outer_no * SWEEPS)
        if first:
            for copy in first_copies:
                copy.wait_recv()
            fracture = gather_ref[0]
        picked = lax.dot_general(fracture, by_block, (((0,), (0,)), ((), ())), precision=EXACT, preferred_element_type=jnp.float32)
        flux = kappa_ref[...] * (trace - jnp.sum(picked * by_lane, axis=0, keepdims=True))
        landed = lax.dot_general(by_block * flux, by_lane, (((1,), (1,)), ((), ())), precision=EXACT, preferred_element_type=jnp.float32)
        if first:
            forward, spread = products(0, True)
        for k in range(n_frac):
            if first:
                outgo_ref[stage, k, 0:rows, :] = spread[k * rows : (k + 1) * rows]
            outgo_ref[stage, k, rows : 2 * rows, :] = landed[k * rows : (k + 1) * rows]
        parts = [lane_hot_ref[...] * part for part in thirds(flux)]
        if first:
            pieces.append(set_inverse)
        for q in range(4):
            pieces.append(functools.partial(set_sources, q * quarter, parts))
        for s in range(SWEEPS):
            add_sweep(outer_no * SWEEPS + s)
        both = exchange(stage, 0 if first else rows, 2 * rows, 2)
        if first:
            image = diag * begin + 0.5 * (forward + both[0:rows])
        mat_ref[outer_no, me_mat] = both[rows:] if first else both
        slot = mat_ref.at[outer_no, me_mat]
        copies = [
            send(slot, slot, mat_send.at[outer_no, k - 1], mat_recv.at[outer_no, k - 1], {"mat": lax.rem(me_mat + k, n_mat)})
            for k in range(1, n_mat)
        ]
        fill(2)
        for copy in copies:
            copy.wait_recv()
        load = mat_ref[outer_no, 0]
        for k in range(1, n_mat):
            load = load + mat_ref[outer_no, k]
        if first:
            residual = fsource_ref[...] + load - image
        else:
            residual = residual + (load - loaded)
        loaded = load

        for step in range(CG_ITERS):
            phase = stage + step + 1
            needed = first or step + 1 < CG_ITERS
            copies = gather(phase, residual)
            fill(2)
            for copy in copies:
                copy.wait_recv()
            whole = gather_ref[phase]
            forward, spread = products(phase, needed)
            inner = residual * (diag * residual + forward)
            for k in range(n_frac):
                if needed:
                    outgo_ref[phase, k, 0:rows, :] = spread[k * rows : (k + 1) * rows]
                outgo_ref[phase, k, rows : 2 * rows, :] = inner
            both = exchange(phase, 0 if needed else rows, 2 * rows, 3)
            if needed:
                image = diag * residual + 0.5 * (forward + both[0:rows])
                product = total_of(both[rows : 2 * rows])
            else:
                product = total_of(both)
            norm_next = total_of(whole * whole)
            if step == 0:
                alpha = norm_next / product
                direction = whole
                along = image
            else:
                ratio = norm_next / norm_now
                alpha = norm_next / (product - ratio * norm_next / alpha)
                direction = whole + ratio * direction
                if needed:
                    along = image + ratio * along
            norm_now = norm_next
            fracture = fracture + alpha * direction
            if needed:
                residual = residual - alpha * along
        fill(len(pieces))
    flux_ref[...] = flux
    gather_ref[phases] = fracture
    own_ref[...] = gather_ref[phases, mine, :]
    for copy in sent:
        copy.wait_send()


def coupled(pressure, face, cell_coef, matrix_source, cells, kappa, place, tiles, tile_cols, diag, begin, fsource):
    n_frac, n_mat = lax.axis_size("frac"), lax.axis_size("mat")
    rows, tiles_row, size_b = tiles.shape[0], tiles.shape[1], tiles.shape[3]
    blocks = rows * n_frac
    x, y, z = pressure.shape
    slots = cells.shape[1]
    f32 = jnp.float32
    vmem = pl.BlockSpec(memory_space=pltpu.VMEM)
    smem = pl.BlockSpec(memory_space=pltpu.SMEM)
    phases = OUTER * (CG_ITERS + 1)
    sweeps = OUTER * SWEEPS
    dma = pltpu.SemaphoreType.DMA
    return pl.pallas_call(
        functools.partial(coupled_kernel, n_frac, n_mat),
        out_shape=(
            jax.ShapeDtypeStruct((x, y, z), f32),
            jax.ShapeDtypeStruct((rows, size_b), f32),
            jax.ShapeDtypeStruct((1, slots), f32),
        ),
        in_specs=[vmem] * 8 + [smem] + [vmem] * 4,
        out_specs=(vmem,) * 3,
        scratch_shapes=[
            pltpu.VMEM((phases, blocks, size_b), f32),
            pltpu.VMEM((phases, n_frac, 2 * rows, size_b), f32),
            pltpu.VMEM((phases, n_frac, 2 * rows, size_b), f32),
            pltpu.VMEM((OUTER, n_mat, rows, size_b), f32),
            pltpu.VMEM((rows * tiles_row, size_b), f32),
            pltpu.VMEM((rows, size_b), f32),
            pltpu.VMEM((sweeps, x + 2, y, z), f32),
            pltpu.VMEM((x + 1, y, z), f32),
            pltpu.VMEM((x, y, z), f32),
            pltpu.VMEM((x, y, z), f32),
            pltpu.VMEM((x * y, slots), jnp.bfloat16),
            pltpu.VMEM((z, slots), jnp.bfloat16),
            pltpu.VMEM((sweeps, 2, x, z), f32),
            pltpu.VMEM((sweeps, 2, x, z), f32),
            pltpu.VMEM((x, z), f32),
            pltpu.VMEM((x, z), f32),
            dma((phases, n_frac - 1)),
            dma((phases, n_frac - 1)),
            dma((phases, n_frac - 1)),
            dma((phases, n_frac - 1)),
            dma((OUTER, n_mat - 1)),
            dma((OUTER, n_mat - 1)),
            dma((sweeps + 1, 4)),
            dma((sweeps + 1, 4)),
        ],
        compiler_params=pltpu.CompilerParams(
            collective_id=0, has_side_effects=True, vmem_limit_bytes=60 * 1024 * 1024
        ),
        name="coupled",
    )(pressure, face, cell_coef, matrix_source, cells, kappa, place, tiles, tile_cols, tile_cols.reshape(1, -1), diag, begin, fsource)


def body(
    pressure_start,
    face_trans,
    cell_coef,
    matrix_source,
    mortar_owner,
    mortar_cell,
    mortar_frac,
    mortar_kappa,
    tiles,
    tile_cols,
    frac_diag,
    frac_source,
    fracture_start,
):
    mat_count = lax.axis_size("mat")
    frac_count = lax.axis_size("frac")
    devices = mat_count * frac_count
    size_b = tiles.shape[2]
    owner = mortar_owner[:, 0]
    mortar_count = owner.shape[0]
    capacity = max(2, 2 * mortar_count // devices)
    hits = (owner[:, None] == jnp.arange(devices, dtype=jnp.int32)[None, :]).astype(jnp.int32)
    ranks = jnp.cumsum(hits, axis=0)
    slot = jnp.sum(ranks * hits, axis=1) - 1
    place = owner * capacity + slot
    slots = devices * capacity
    at_slot = (place[:, None] == jnp.arange(slots, dtype=jnp.int32)[None, :]).astype(jnp.float32)
    payload = jnp.stack([mortar_cell.astype(jnp.float32), mortar_frac.astype(jnp.float32), mortar_kappa])
    outgoing = jnp.dot(payload, at_slot, precision=EXACT).reshape(3, devices, capacity)
    incoming = lax.all_to_all(outgoing, ("mat", "frac"), split_axis=1, concat_axis=1, tiled=True)
    cell_slots = jnp.round(incoming[0]).astype(jnp.int32).reshape(1, -1)
    frac_slots = jnp.round(incoming[1]).astype(jnp.int32).reshape(1, -1)
    kappa_slots = incoming[2].reshape(1, -1)
    blocked = (-1, size_b)
    pressure, fracture, flux = coupled(
        pressure_start,
        face_trans,
        cell_coef,
        matrix_source,
        cell_slots,
        kappa_slots,
        frac_slots,
        tiles,
        tile_cols,
        frac_diag.reshape(blocked),
        fracture_start.reshape(blocked),
        frac_source.reshape(blocked),
    )
    returned = lax.all_to_all(
        flux.reshape(devices, capacity), ("mat", "frac"), split_axis=0, concat_axis=0, tiled=True
    )
    return (pressure, fracture.reshape(-1), returned.reshape(-1)[place])


def solution(mesh):
    in_specs = (
        P("mat", "frac", None),
        P(None, "mat", "frac", None),
        P("mat", "frac", None),
        P("mat", "frac", None),
        P(("mat", "frac"), None),
        P(("mat", "frac")),
        P(("mat", "frac")),
        P(("mat", "frac")),
        P("frac", None, None, None),
        P("frac", None),
        P("frac"),
        P("frac"),
        P("frac"),
    )
    out_specs = (P("mat", "frac", None), P("frac"), P(("mat", "frac")))
    return jax.shard_map(body, mesh=mesh, in_specs=in_specs, out_specs=out_specs, check_vma=False)
```
